256 devices in a mesh: row: 32 (over x, z_lo, y), col: 8 (over z_hi, core).
Axes of the slice: x: 4, y: 4, z: 8 (z_hi: 4, z_lo: 2; z = z_hi * 2 + z_lo), core: 2. Of those that a mesh axis runs over, the one named last changes fastest.
Arguments:
- adj_tiles: bfloat16 [32, 8, 128, 128, 128], P('row', 'col'), may hold values from 0 to 1, as said below
- tile_rows: int32 [32, 8, 128], P('row', 'col'), may hold values from 0 to 7, as said below
- tile_cols: int32 [32, 8, 128], P('row', 'col'), may hold values from 0 to 31, as said below
- tile_count: int32 [32, 8], P('row', 'col'), may hold values from 1 to 128, as said below
- tile_depth: int32 [256, 128], P(('row', 'col')), may hold values from 1 to 7, as said below
- source_ids: int32 [128], replicated, may hold values from 0 to 32767
Outputs:
- path_sums: float32 [32768, 128], P(('row', 'col'))
- log_scales: float32 [6, 128], replicated
The draws below stay inside these ranges and needn't reach their ends.
Inputs may be any that keep to these rules, and one draw needn't show every extreme that they name: `adj_tiles`: every entry is 0 or 1. The live slots of a device are its first tile_count slots; at least one device holds 128 live slots. `tile_rows`: slots past a device's live count carry 0. `tile_cols`: slots past a device's live count carry 0. `tile_depth`: the value 6 + 1 marks a tile that takes path counts at every level.
All inputs are finite; a program needn't handle non-finite values.
Results may differ from the reference program's by a relative error of at most 0.0003.
Values may be sent and summed in bfloat16 or wider, within the bound.
No kernel may reach another device: no remote copies, remote signals or barrier semaphores. Data moves between devices by JAX's collectives and lax.ppermute only.
A program may use at most 64 MiB of HBM per device.

```python
import jax
import jax.numpy as jnp
from jax import lax

TILE = 128
PANEL = 128
PIECE = 128
KMAX = 128
LEVELS = 6
VERTICES = 32768
VTILES = 256
DEST_TILES = 8
SRC_TILES = 32
N_ROW = 32
N_COL = 8


def tile_lists(key):
    grid_shape = (N_ROW, N_COL)
    light = jax.random.randint(jax.random.fold_in(key, 11), grid_shape, KMAX // 4, KMAX // 2 + 1)
    heavy = jax.random.randint(jax.random.fold_in(key, 12), grid_shape, 0, 4) == 0
    loaded = jax.random.randint(jax.random.fold_in(key, 13), grid_shape, 3 * KMAX // 4, KMAX + 1)
    counts = jnp.where(heavy, loaded, light)
    chosen = jax.random.randint(jax.random.fold_in(key, 14), (), 0, N_ROW * N_COL)
    device_ids = jnp.arange(N_ROW * N_COL, dtype=jnp.int32).reshape(grid_shape)
    counts = jnp.where(device_ids == chosen, KMAX, counts).astype(jnp.int32)
    slot_ids = jnp.arange(KMAX, dtype=jnp.int32)[None, None, :]
    live_slots = slot_ids < counts[:, :, None]
    dest_ids = jax.random.randint(jax.random.fold_in(key, 15), grid_shape + (KMAX,), 0, DEST_TILES)
    src_ids = jax.random.randint(jax.random.fold_in(key, 16), grid_shape + (KMAX,), 0, SRC_TILES)
    dest_ids = jnp.where(live_slots, dest_ids, 0).astype(jnp.int32)
    src_ids = jnp.where(live_slots, src_ids, 0).astype(jnp.int32)
    return (counts, dest_ids, src_ids)


def draw_adj_tiles(key, part):
    counts, dest_ids, src_ids = tile_lists(key)
    piece_tiles = PIECE // TILE
    row_index = jnp.arange(N_ROW, dtype=jnp.int32)[:, None, None]
    col_index = jnp.arange(N_COL, dtype=jnp.int32)[None, :, None]
    dest_global = (row_index * (N_COL * piece_tiles) + dest_ids).astype(jnp.int32)
    src_global = ((src_ids // piece_tiles * N_COL + col_index) * piece_tiles + src_ids % piece_tiles).astype(jnp.int32)
    log_weight = jax.random.uniform(jax.random.fold_in(key, 33), (VTILES, TILE), jnp.float32, jnp.log(0.3), jnp.log(1.0))
    vertex_weight = jnp.exp(log_weight)
    dest_weight = jnp.take(vertex_weight, dest_global, axis=0)
    src_weight = jnp.take(vertex_weight, src_global, axis=0)
    pair_weight = dest_weight[:, :, :, :, None] * src_weight[:, :, :, None, :]
    slot_shape = (N_ROW, N_COL, KMAX, 1, 1)
    log_density = jax.random.uniform(jax.random.fold_in(key, 31), slot_shape, jnp.float32, jnp.log(0.15), jnp.log(0.6))
    density = jnp.exp(log_density)
    offset = jax.random.randint(jax.random.fold_in(key, 34), slot_shape, 0, TILE)
    positions = jnp.arange(TILE, dtype=jnp.int32)
    spread = positions[None, :] - positions[:, None]
    inside = (spread[None, None, None, :, :] - offset) % TILE < TILE // 4
    rate = jnp.where(inside, jnp.minimum(1.0, 4.0 * density * pair_weight), 0.15 * pair_weight)
    coins = jax.random.uniform(jax.random.fold_in(key, 32), (N_ROW, N_COL, KMAX, TILE, TILE), jnp.float32)
    return (coins < rate).astype(jnp.float32).astype(jnp.bfloat16)


def draw_tile_count(key, part):
    return tile_lists(key)[0]


def draw_tile_rows(key, part):
    return tile_lists(key)[1]


def draw_tile_cols(key, part):
    return tile_lists(key)[2]


def draw_tile_depth(key, part):
    base_level = jax.random.randint(jax.random.fold_in(key, 21), (VTILES, 1), 0, LEVELS + 1)
    offset = jax.random.randint(jax.random.fold_in(key, 22), (VTILES, PANEL), 0, LEVELS + 1)
    return (1 + jnp.maximum(base_level, offset)).astype(jnp.int32)


def place_ends(values, own_key, low, largest):
    longest = values.shape.index(max(values.shape))
    spots = []
    for shift in (0, 1):
        where = [jax.random.randint(jax.random.fold_in(own_key, axis), (), 0, length) for axis, length in enumerate(values.shape)]
        where[longest] = (where[longest] + shift) % values.shape[longest]
        spots.append(tuple(where))
    return values.at[spots[0]].set(low).at[spots[1]].set(largest)


def setup_inputs(seed: int = 0) -> dict:
    keys = jax.random.split(jax.random.key(seed), 7)
    adj_tiles = draw_adj_tiles(jax.random.fold_in(keys[6], 71), 0)
    tile_rows = draw_tile_rows(jax.random.fold_in(keys[6], 71), 0)
    tile_cols = draw_tile_cols(jax.random.fold_in(keys[6], 71), 0)
    tile_count = draw_tile_count(jax.random.fold_in(keys[6], 71), 0)
    tile_depth = draw_tile_depth(jax.random.fold_in(keys[6], 71), 0)
    source_ids = place_ends(jax.random.randint(keys[5], (PANEL,), 0, VERTICES), jax.random.fold_in(keys[5], 1), 0, VERTICES - 1).astype(jnp.int32)
    return dict(adj_tiles=adj_tiles, tile_rows=tile_rows, tile_cols=tile_cols, tile_count=tile_count, tile_depth=tile_depth, source_ids=source_ids)


EPSILON = 1e-06

def reference(adj_tiles, tile_rows, tile_cols, tile_count, tile_depth, source_ids):
    piece_tiles = PIECE // TILE
    tile_total = VERTICES // TILE
    row_slots = N_COL * KMAX
    slot_ids = jnp.arange(KMAX, dtype=jnp.int32)[None, None, :]
    row_index = jnp.arange(N_ROW, dtype=jnp.int32)[:, None, None]
    col_index = jnp.arange(N_COL, dtype=jnp.int32)[None, :, None]
    dest_tile = (row_index * (N_COL * piece_tiles) + tile_rows).reshape(-1).astype(jnp.int32)
    src_tile = ((tile_cols // piece_tiles * N_COL + col_index) * piece_tiles + tile_cols % piece_tiles).reshape(-1).astype(jnp.int32)
    live_slots = (slot_ids < tile_count[:, :, None]).astype(jnp.float32).reshape(-1)
    flat_tiles = adj_tiles.reshape(N_ROW * row_slots, TILE, TILE)

    def product(frontier):

        def one_row(summed, row_number):
            first_slot = (row_number * row_slots).astype(jnp.int32)
            block_part = lax.dynamic_slice_in_dim(flat_tiles, first_slot, row_slots, 0).astype(jnp.float32)
            dest_part = lax.dynamic_slice_in_dim(dest_tile, first_slot, row_slots, 0)
            src_part = lax.dynamic_slice_in_dim(src_tile, first_slot, row_slots, 0)
            weights = lax.dynamic_slice_in_dim(live_slots, first_slot, row_slots, 0)
            picked = jnp.take(frontier, src_part, axis=0).astype(jnp.float32)
            slot_terms = jnp.einsum('kij,kjs->kis', block_part, picked, precision=lax.Precision.HIGHEST)
            slot_terms = slot_terms * weights[:, None, None]
            return (summed.at[dest_part].add(slot_terms), None)
        zero_sums = jnp.zeros((tile_total, TILE, PANEL), jnp.float32)
        summed, unused = lax.scan(one_row, zero_sums, jnp.arange(N_ROW, dtype=jnp.int32))
        return summed
    vertex_ids = jnp.arange(VERTICES, dtype=jnp.int32)
    start_panel = (vertex_ids[:, None] == source_ids[None, :]).astype(jnp.float32)
    path_sums = start_panel
    frontier = start_panel.astype(jnp.bfloat16)
    log_scales = []
    for level_index in range(1, LEVELS + 1):
        summed = product(frontier.reshape(tile_total, TILE, PANEL))
        reached = (tile_depth >= level_index).astype(jnp.float32)
        raw_paths = (summed * reached[:, None, :]).reshape(VERTICES, PANEL)
        mean_square = lax.optimization_barrier(jnp.sum(raw_paths * raw_paths, axis=0)) / VERTICES + EPSILON
        scaled = raw_paths * lax.rsqrt(mean_square)
        path_sums = path_sums + scaled
        log_scales.append(0.5 * jnp.log(mean_square))
        frontier = scaled.astype(jnp.bfloat16)
    return (path_sums, jnp.stack(log_scales))
```

```python
import jax
import jax.numpy as jnp
from jax import lax
from jax.experimental import pallas as pl
from jax.experimental.pallas import tpu as pltpu
from jax.sharding import Mesh
from jax.sharding import PartitionSpec as P

TILE = 128
PANEL = 128
LEVELS = 6
KMAX = 128
DEST_TILES = 8
SRC_TILES = 32
VERTICES = 32768
EPSILON = 1e-06
ROW = ("row_0", "row_1", "row_2")
COL = ("col_0", "col_1")
ROW_COL = ROW + COL
GROUP = 4
LIST_LEN = KMAX + DEST_TILES * GROUP
EXTRA = 8
ROWS = TILE + EXTRA


def f32(x):
    return x.astype(jnp.float32)


def sort_kernel(rows, cols, count, order, starts, fill):
    live = count[0]
    for d in range(DEST_TILES):
        fill[d] = 0

    def tally(k, carry):
        d = rows[k]
        fill[d] = fill[d] + 1
        return carry

    lax.fori_loop(0, live, tally, 0)
    first = jnp.int32(0)
    for d in range(DEST_TILES):
        held = fill[d]
        starts[d] = first
        fill[d] = first * GROUP
        first = first + (held + GROUP - 1) // GROUP
    starts[DEST_TILES] = first

    def blank(i, carry):
        order[i] = SRC_TILES * KMAX
        return carry

    lax.fori_loop(0, first * GROUP, blank, 0)

    def place(k, carry):
        d = rows[k]
        i = fill[d]
        order[i] = cols[k] * KMAX + k
        fill[d] = i + 1
        return carry

    lax.fori_loop(0, live, place, 0)


def sort_slots(rows, cols, count):
    smem = pl.BlockSpec(memory_space=pltpu.SMEM)
    return pl.pallas_call(
        sort_kernel,
        in_specs=[smem, smem, smem],
        out_specs=[smem, smem],
        out_shape=[
            jax.ShapeDtypeStruct((LIST_LEN,), jnp.int32),
            jax.ShapeDtypeStruct((16,), jnp.int32),
        ],
        scratch_shapes=[pltpu.SMEM((DEST_TILES,), jnp.int32)],
        name="sort_slots",
    )(rows, cols, count)


def product_kernel(order, starts, place, adj, sources, away, kept, held):
    c0, c1 = place[0], place[1]
    parts = jnp.sum(f32(sources[:, TILE:ROWS, :]), axis=0)
    squares = (parts[0:1] + parts[1:2]) + parts[2:3]
    row = lax.broadcasted_iota(jnp.int32, (EXTRA, PANEL), 0)
    extra = jnp.where(row == c0 * 2 + c1, jnp.broadcast_to(squares, (EXTRA, PANEL)), 0.0)
    for t in range(SRC_TILES):
        held[t] = sources[t, 0:TILE, :]
    held[SRC_TILES] = jnp.zeros((TILE, PANEL), jnp.bfloat16)

    for out, core in ((away, 1 - c1), (kept, c1)):
        for k in range(4):
            d = lax.rem(c0 + k, 4) * 2 + core

            def turn(g, total):
                lefts, rights = [], []
                for i in range(GROUP):
                    code = order[g * GROUP + i]
                    lefts.append(adj[code & (KMAX - 1)])
                    rights.append(held[lax.shift_right_logical(code, 7)])
                left = jnp.concatenate(lefts, axis=1)
                right = jnp.concatenate(rights, axis=0)
                return total + jnp.dot(left, right, preferred_element_type=jnp.float32)

            total = lax.fori_loop(
                starts[d], starts[d + 1], turn, jnp.zeros((TILE, PANEL), jnp.float32)
            )
            out[k, 0:TILE, :] = total
            out[k, TILE:ROWS, :] = extra


def products(order, starts, place, adj, sources):
    smem = pl.BlockSpec(memory_space=pltpu.SMEM)
    vmem = pl.BlockSpec(memory_space=pltpu.VMEM)
    chunk = jax.ShapeDtypeStruct((4, ROWS, PANEL), jnp.float32)
    return pl.pallas_call(
        product_kernel,
        in_specs=[smem, smem, smem, vmem, vmem],
        out_specs=[vmem, vmem],
        out_shape=[chunk, chunk],
        scratch_shapes=[pltpu.VMEM((SRC_TILES + 1, TILE, PANEL), jnp.bfloat16)],
        compiler_params=pltpu.CompilerParams(vmem_limit_bytes=16 * 1024 * 1024),
        name="products",
    )(order, starts, place, adj, sources)


def split3(x):
    high = x.astype(jnp.bfloat16)
    rest = x - f32(high)
    middle = rest.astype(jnp.bfloat16)
    low = (rest - f32(middle)).astype(jnp.bfloat16)
    return f32(high), f32(middle), f32(low)


def level_kernel(level, own, one, two, three, depth, raw_in, sums_in, sums, raw, squares, scale, spread):
    total = (own[...] + one[...]) + (two[...] + three[...])
    product = total[0:TILE]
    reached = depth[...] >= level
    if level == 1:
        sums[...] = sums_in[...]
        scale[...] = jnp.zeros((1, PANEL), jnp.float32)
    else:
        mean_square = jnp.sum(total[TILE:ROWS], axis=0, keepdims=True) / VERTICES + EPSILON
        scale[...] = mean_square
        inverse = lax.rsqrt(mean_square)
        sums[...] = sums_in[...] + raw_in[...] * inverse
        product = product * inverse
    paths = jnp.where(reached, product, 0.0)
    raw[...] = paths
    square = jnp.sum(paths * paths, axis=0, keepdims=True)
    squares[...] = square
    if level < LEVELS:
        sent = paths.astype(jnp.bfloat16)
        high, middle, low = split3(square)
        row = lax.broadcasted_iota(jnp.int32, (EXTRA, PANEL), 0)
        extra = jnp.where(
            row == 0, high, jnp.where(row == 1, middle, jnp.where(row == 2, low, 0.0))
        ).astype(jnp.bfloat16)
        for t in range(SRC_TILES):
            spread[t, 0:TILE, :] = sent
            spread[t, TILE:ROWS, :] = extra
    else:
        spread[...] = jnp.zeros(spread.shape, spread.dtype)


def finish_level(level, chunks, depth, raw, sums):
    vmem = pl.BlockSpec(memory_space=pltpu.VMEM)
    panel = jax.ShapeDtypeStruct((TILE, PANEL), jnp.float32)
    line = jax.ShapeDtypeStruct((1, PANEL), jnp.float32)
    spread_tiles = SRC_TILES if level < LEVELS else 1
    return pl.pallas_call(
        lambda *refs: level_kernel(level, *refs),
        in_specs=[vmem] * 7,
        out_specs=[vmem] * 5,
        out_shape=[
            panel,
            panel,
            line,
            line,
            jax.ShapeDtypeStruct((spread_tiles, ROWS, PANEL), jnp.bfloat16),
        ],
        compiler_params=pltpu.CompilerParams(vmem_limit_bytes=16 * 1024 * 1024),
        name=f"level_{level}",
    )(*chunks, depth, raw, sums)


def shifted(x, axis, count, step):
    return lax.ppermute(x, axis, [(i, (i + step) % count) for i in range(count)])


def summed_alike(x, axis, count):
    if count == 2:
        return x + shifted(x, axis, 2, 1)
    mine = jnp.arange(count, dtype=jnp.int32)[:, None] == lax.axis_index(axis)
    slots = jnp.where(mine, x, 0.0)
    slots = slots + sum(shifted(slots, axis, count, k) for k in range(1, count))
    return in_order(slots, count)


def in_order(slots, count):
    total = slots[0:1]
    for i in range(1, count):
        total = total + slots[i : i + 1]
    return total


def local(adj_tiles, tile_rows, tile_cols, tile_count, tile_depth, source_ids):
    adj = adj_tiles[0, 0]
    c0, c1 = lax.axis_index("col_0"), lax.axis_index("col_1")
    column = lax.axis_index(COL)
    position = lax.axis_index(ROW) * DEST_TILES + column
    order, starts = sort_slots(tile_rows[0, 0], tile_cols[0, 0], tile_count[0])
    place = jnp.stack([c0, c1]).astype(jnp.int32)
    vertex = position * TILE + jnp.arange(TILE, dtype=jnp.int32)
    sums = f32(vertex[:, None] == source_ids[None, :])
    raw = sums
    tile = jnp.arange(SRC_TILES, dtype=jnp.int32)[:, None, None]
    inner = jnp.arange(ROWS, dtype=jnp.int32)[None, :, None]
    vertex = jnp.where(inner < TILE, (tile * DEST_TILES + column) * TILE + inner, -1)
    sources = (vertex == source_ids[None, None, :]).astype(jnp.bfloat16)
    scales = []
    for level in range(1, LEVELS + 1):
        away, kept = products(order, starts, place, adj, sources)
        kept = kept + shifted(away, "col_1", 2, 1)
        moved = {k: shifted(kept[k], "col_0", 4, k) for k in (2, 1, 3)}
        chunks = (kept[0], moved[1], moved[2], moved[3])
        sums, raw, squares, scale, spread = finish_level(level, chunks, tile_depth, raw, sums)
        if level > 1:
            scales.append(scale)
        if level < LEVELS:
            sources = lax.all_to_all(spread, ROW, 0, 0, tiled=True)
    total = squares
    for axis, count in (("col_1", 2), ("col_0", 4), ("row_0", 4), ("row_1", 2), ("row_2", 4)):
        total = summed_alike(total, axis, count)
    mean_square = total / VERTICES + EPSILON
    scales.append(mean_square)
    path_sums = sums + raw * lax.rsqrt(mean_square)
    return path_sums, 0.5 * jnp.log(jnp.concatenate(scales, axis=0))


def solution(mesh):
    split = Mesh(mesh.devices.reshape(4, 2, 4, 4, 2), ROW_COL)
    in_specs = (
        P(ROW, COL, None, None, None),
        P(ROW, COL, None),
        P(ROW, COL, None),
        P(ROW, COL),
        P(ROW_COL, None),
        P(),
    )
    out_specs = (P(ROW_COL, None), P())
    return jax.shard_map(local, mesh=split, in_specs=in_specs, out_specs=out_specs, check_vma=False)
```

```python
import jax
import jax.numpy as jnp
from jax import lax
from jax.experimental import pallas as pl
from jax.experimental.pallas import tpu as pltpu
from jax.sharding import Mesh
from jax.sharding import PartitionSpec as P

TILE = 128
PANEL = 128
LEVELS = 6
KMAX = 128
DEST_TILES = 8
SRC_TILES = 32
VERTICES = 32768
EPSILON = 1e-06
ROW = ("row_0", "row_1", "row_2")
COL = ("col_0", "col_1")
ROW_COL = ROW + COL
HALF = TILE // 2
EXTRA = 8
ROWS = TILE + EXTRA
CODED = HALF + EXTRA
TOP = 65535.0
FETCH = 16
DEPTH = 1024
SMEM = pl.BlockSpec(memory_space=pltpu.SMEM)
VMEM = pl.BlockSpec(memory_space=pltpu.VMEM)
LIMIT = pltpu.CompilerParams(vmem_limit_bytes=24 * 1024 * 1024)


def f32(x):
    return x.astype(jnp.float32)


def multiply(dense, held, extra, out):
    for k in range(4):
        out[k, 0:TILE, :] = jnp.zeros((TILE, PANEL), jnp.float32)
        out[k, TILE:ROWS, :] = extra[...]

    def turn(n, carry):
        part = pl.ds(pl.multiple_of(n * DEPTH, DEPTH), DEPTH)
        product = jnp.dot(dense[:, part], held[part, :], preferred_element_type=jnp.float32)
        for k in range(4):
            out[k, 0:TILE, :] = out[k, 0:TILE, :] + product[k * TILE : (k + 1) * TILE]
        return carry

    lax.fori_loop(0, SRC_TILES * TILE // DEPTH, turn, 0)


def first_kernel(
    rows, cols, place, ids, adj, away_out, kept_out, away_dense, kept_dense,
    away, kept, staged, held, extra, sems, stores,
):
    live, c1 = place[0], place[2]

    def fetch(n):
        part = pl.ds(n * FETCH, FETCH)
        return pltpu.make_async_copy(adj.at[part], staged.at[part], sems.at[n])

    for n in range(KMAX // FETCH):

        @pl.when(n * FETCH < live)
        def _(n=n):
            fetch(n).start()

    def clear(i, carry):
        part = pl.ds(pl.multiple_of(i * TILE, TILE), TILE)
        blank = jnp.zeros((TILE, SRC_TILES * TILE), jnp.bfloat16)
        away[part, :] = blank
        kept[part, :] = blank
        return carry

    lax.fori_loop(0, DEST_TILES // 2, clear, 0)
    column = place[1] * 2 + c1
    inner = lax.broadcasted_iota(jnp.int32, (TILE, PANEL), 0)
    wanted = jnp.broadcast_to(ids[...], (TILE, PANEL)) - inner
    for t in range(SRC_TILES):
        hit = wanted == (t * DEST_TILES + column) * TILE
        held[t * TILE : (t + 1) * TILE, :] = jnp.where(hit, 1.0, 0.0).astype(jnp.bfloat16)
    extra[...] = jnp.zeros((EXTRA, PANEL), jnp.float32)

    def add(k, carry):
        d, u = rows[k], cols[k]
        down = pl.ds(pl.multiple_of((d >> 1) * TILE, TILE), TILE)
        across = pl.ds(pl.multiple_of(u * TILE, TILE), TILE)

        @pl.when((d & 1) == c1)
        def _():
            kept[down, across] = kept[down, across] + staged[k]

        @pl.when((d & 1) != c1)
        def _():
            away[down, across] = away[down, across] + staged[k]

        return carry

    for n in range(KMAX // FETCH):

        @pl.when(n * FETCH < live)
        def _(n=n):
            fetch(n).wait()
            lax.fori_loop(n * FETCH, jnp.minimum(live, (n + 1) * FETCH), add, 0)

    pairs = ((away, away_dense), (kept, kept_dense))
    copies = [pltpu.make_async_copy(v, h, stores.at[i]) for i, (v, h) in enumerate(pairs)]
    for copy in copies:
        copy.start()
    multiply(away, held, extra, away_out)
    multiply(kept, held, extra, kept_out)
    for copy in copies:
        copy.wait()


def first_products(rows, cols, place, ids, adj):
    hbm = pl.BlockSpec(memory_space=pltpu.HBM)
    half = (DEST_TILES // 2 * TILE, SRC_TILES * TILE)
    chunks = jax.ShapeDtypeStruct((4, ROWS, PANEL), jnp.float32)
    dense = jax.ShapeDtypeStruct(half, jnp.bfloat16)
    return pl.pallas_call(
        first_kernel,
        in_specs=[SMEM, SMEM, SMEM, VMEM, hbm],
        out_specs=[VMEM, VMEM, hbm, hbm],
        out_shape=[chunks, chunks, dense, dense],
        scratch_shapes=[
            pltpu.VMEM(half, jnp.bfloat16),
            pltpu.VMEM(half, jnp.bfloat16),
            pltpu.VMEM((KMAX, TILE, TILE), jnp.bfloat16),
            pltpu.VMEM((SRC_TILES * TILE, PANEL), jnp.bfloat16),
            pltpu.VMEM((EXTRA, PANEL), jnp.float32),
            pltpu.SemaphoreType.DMA((KMAX // FETCH,)),
            pltpu.SemaphoreType.DMA((2,)),
        ],
        compiler_params=LIMIT,
        name="first_products",
    )(rows, cols, place, ids, pltpu.with_memory_space_constraint(adj, pltpu.HBM))


def away_kernel(place, dense, sources, out, held, extra):
    parts = jnp.sum(f32(sources[:, TILE:ROWS, :]), axis=0)
    squares = (parts[0:1] + parts[1:2]) + parts[2:3]
    row = lax.broadcasted_iota(jnp.int32, (EXTRA, PANEL), 0)
    extra[...] = jnp.where(row == place[2], jnp.broadcast_to(squares, (EXTRA, PANEL)), 0.0)
    for t in range(SRC_TILES):
        held[t * TILE : (t + 1) * TILE, :] = sources[t, 0:TILE, :]
    multiply(dense, held, extra, out)


def away_products(place, dense, sources):
    return pl.pallas_call(
        away_kernel,
        in_specs=[SMEM, VMEM, VMEM],
        out_specs=[VMEM] * 3,
        out_shape=[
            jax.ShapeDtypeStruct((4, ROWS, PANEL), jnp.float32),
            jax.ShapeDtypeStruct((SRC_TILES * TILE, PANEL), jnp.bfloat16),
            jax.ShapeDtypeStruct((EXTRA, PANEL), jnp.float32),
        ],
        compiler_params=LIMIT,
        name="away_products",
    )(place, dense, sources)


def kept_products(dense, held, extra):
    return pl.pallas_call(
        multiply,
        in_specs=[VMEM] * 3,
        out_specs=VMEM,
        out_shape=jax.ShapeDtypeStruct((4, ROWS, PANEL), jnp.float32),
        compiler_params=LIMIT,
        name="kept_products",
    )(dense, held, extra)


def as_integers(x):
    x = jnp.maximum(x, 2.0**-80)
    exponent = jnp.floor(jnp.log2(x)) - 22.0
    return jnp.floor(x * jnp.exp2(-exponent) + 0.5), exponent


def encode_kernel(kept, away, coded):
    row = lax.broadcasted_iota(jnp.int32, (EXTRA, PANEL), 0)
    for k in range(4):
        total = kept[k] + away[k]
        sums = total[0:TILE]
        lines = list(as_integers(jnp.max(sums, axis=0, keepdims=True)))
        factor = TOP / (lines[0] * jnp.exp2(lines[1]))
        codes = jnp.minimum(jnp.floor(sums * factor + 0.5), TOP).astype(jnp.int32)
        coded[k, 0:HALF, :] = lax.shift_left(codes[0:HALF], 16) | codes[HALF:TILE]
        lines += as_integers(total[TILE : TILE + 1])
        lines += as_integers(total[TILE + 1 : TILE + 2])
        tail = jnp.zeros((EXTRA, PANEL), jnp.float32)
        for n, line in enumerate(lines):
            tail = jnp.where(row == n, jnp.broadcast_to(line, (EXTRA, PANEL)), tail)
        coded[k, HALF:CODED, :] = tail.astype(jnp.int32)


def encoded(kept, away):
    return pl.pallas_call(
        encode_kernel,
        in_specs=[VMEM] * 2,
        out_specs=VMEM,
        out_shape=jax.ShapeDtypeStruct((4, CODED, PANEL), jnp.int32),
        compiler_params=LIMIT,
        name="encoded",
    )(kept, away)


def split3(x):
    high = f32(x.astype(jnp.bfloat16))
    rest = x - high
    middle = f32(rest.astype(jnp.bfloat16))
    return high, middle, rest - middle


def level_kernel(level, coded, depth, raw_in, sums_in, sums, raw, squares, scale, *spread):
    highs = jnp.zeros((HALF, PANEL), jnp.float32)
    lows = jnp.zeros((HALF, PANEL), jnp.float32)
    mean_square = jnp.zeros((1, PANEL), jnp.float32)
    for k in range(4):
        tail = f32(coded[k, HALF:CODED, :])
        power = jnp.exp2(jnp.minimum(tail, 127.0))
        step = tail[0:1] * power[1:2] * (1.0 / TOP)
        mean_square = mean_square + tail[2:3] * power[3:4]
        mean_square = mean_square + tail[4:5] * power[5:6]
        codes = coded[k, 0:HALF, :]
        highs = highs + f32(lax.shift_right_logical(codes, 16)) * step
        lows = lows + f32(codes & 65535) * step
    product = jnp.concatenate([highs, lows], axis=0)
    reached = depth[...] >= level
    if level == 1:
        sums[...] = sums_in[...]
        scale[...] = jnp.zeros((1, PANEL), jnp.float32)
    else:
        mean_square = mean_square / VERTICES + EPSILON
        scale[...] = mean_square
        inverse = lax.rsqrt(mean_square)
        sums[...] = sums_in[...] + raw_in[...] * inverse
        product = product * inverse
    paths = jnp.where(reached, product, 0.0)
    raw[...] = paths
    square = jnp.sum(paths * paths, axis=0, keepdims=True)
    squares[...] = square
    if level < LEVELS:
        row = lax.broadcasted_iota(jnp.int32, (EXTRA, PANEL), 0)
        tail = jnp.zeros((EXTRA, PANEL), jnp.float32)
        for n, line in enumerate(split3(square)):
            tail = jnp.where(row == n, jnp.broadcast_to(line, (EXTRA, PANEL)), tail)
        sent, tail = paths.astype(jnp.bfloat16), tail.astype(jnp.bfloat16)
        for t in range(SRC_TILES):
            spread[0][t, 0:TILE, :] = sent
            spread[0][t, TILE:ROWS, :] = tail


def finish_level(level, chunks, depth, raw, sums):
    panel = jax.ShapeDtypeStruct((TILE, PANEL), jnp.float32)
    line = jax.ShapeDtypeStruct((1, PANEL), jnp.float32)
    spread = jax.ShapeDtypeStruct((SRC_TILES, ROWS, PANEL), jnp.bfloat16)
    shapes = [panel, panel, line, line] + ([spread] if level < LEVELS else [])
    return pl.pallas_call(
        lambda *refs: level_kernel(level, *refs),
        in_specs=[VMEM] * 4,
        out_specs=[VMEM] * len(shapes),
        out_shape=shapes,
        compiler_params=LIMIT,
        name=f"level_{level}",
    )(chunks, depth, raw, sums)


def from_partner(x):
    return lax.ppermute(x, "col_1", [(0, 1), (1, 0)])


def summed_alike(x, axes):
    copies = jnp.broadcast_to(x, (lax.axis_size(axes), EXTRA, PANEL))
    return jnp.sum(lax.all_to_all(copies, axes, 0, 0, tiled=True)[:, 0], axis=0, keepdims=True)


def local(adj_tiles, tile_rows, tile_cols, tile_count, tile_depth, source_ids):
    position = lax.axis_index(ROW) * DEST_TILES + lax.axis_index(COL)
    place = jnp.stack([tile_count[0, 0], lax.axis_index("col_0"), lax.axis_index("col_1")])
    away, kept, away_dense, kept_dense = first_products(
        tile_rows[0, 0], tile_cols[0, 0], place, source_ids[None, :], adj_tiles[0, 0]
    )
    vertex = position * TILE + jnp.arange(TILE, dtype=jnp.int32)
    sums = f32(vertex[:, None] == source_ids[None, :])
    raw = sums
    scales = []
    for level in range(1, LEVELS + 1):
        if level > 1:
            sources = lax.all_to_all(spread[0], ROW, 0, 0, tiled=True)
            away, held, extra = away_products(place, away_dense, sources)
            kept = kept_products(kept_dense, held, extra)
        coded = encoded(kept, from_partner(away))
        coded = lax.all_to_all(coded, "col_0", 0, 0, tiled=True)
        sums, raw, squares, scale, *spread = finish_level(level, coded, tile_depth, raw, sums)
        if level > 1:
            scales.append(scale)
    total = summed_alike(summed_alike(squares, ("row_1",) + COL), ("row_0", "row_2"))
    mean_square = total / VERTICES + EPSILON
    scales.append(mean_square)
    path_sums = sums + raw * lax.rsqrt(mean_square)
    return path_sums, 0.5 * jnp.log(jnp.concatenate(scales, axis=0))


def solution(mesh):
    split = Mesh(mesh.devices.reshape(4, 2, 4, 4, 2), ROW_COL)
    in_specs = (
        P(ROW, COL, None, None, None),
        P(ROW, COL, None),
        P(ROW, COL, None),
        P(ROW, COL),
        P(ROW_COL, None),
        P(),
    )
    out_specs = (P(ROW_COL, None), P())
    return jax.shard_map(local, mesh=split, in_specs=in_specs, out_specs=out_specs, check_vma=False)
```

```python
import jax
import jax.numpy as jnp
from jax import lax
from jax.experimental import pallas as pl
from jax.experimental.pallas import tpu as pltpu
from jax.sharding import Mesh
from jax.sharding import PartitionSpec as P

TILE = 128
PANEL = 128
LEVELS = 6
KMAX = 128
DEST_TILES = 8
SRC_TILES = 32
VERTICES = 32768
EPSILON = 1e-06
ROW = ("row_0", "row_1", "row_2")
COL = ("col_0", "col_1")
ROW_COL = ROW + COL
SPLIT = (4, 2, 4, 4, 2)
HALF = TILE // 2
EXTRA = 8
ROWS = TILE + EXTRA
CODED = HALF + EXTRA
AWAY = DEST_TILES // 2 * TILE
TOP = 65535.0
ORDER = (1, 3, 2)
FETCH = 16
VMEM = pl.BlockSpec(memory_space=pltpu.VMEM)
WIDE = pltpu.CompilerParams(vmem_limit_bytes=16 * 1024 * 1024)
LIMIT = pltpu.CompilerParams(vmem_limit_bytes=4 * 1024 * 1024)


def f32(x):
    return x.astype(jnp.float32)


def multiply(dense, held, extra, out):
    product = jnp.dot(dense[...], held[...], preferred_element_type=jnp.float32)
    for k in range(4):
        out[k, 0:TILE, :] = product[k * TILE : (k + 1) * TILE]
        out[k, TILE:ROWS, :] = extra[...]


def first_kernel(
    count, rows_in, cols_in, ids_in, adj, away_out, kept_out, dense,
    rows, cols, ids, staged, held, extra, sems, stores,
):
    c1 = lax.axis_index("col_1")

    def fetch(n):
        part = pl.ds(n * FETCH, FETCH)
        return pltpu.make_async_copy(adj.at[part], staged.at[part], sems.at[n])

    small = [
        pltpu.make_async_copy(source, target, stores.at[i])
        for i, (source, target) in enumerate(((ids_in, ids), (rows_in, rows), (cols_in, cols)))
    ]
    for copy in small:
        copy.start()
    live = count[0, 0]
    for n in range(KMAX // FETCH):

        @pl.when(n * FETCH < live)
        def _(n=n):
            fetch(n).start()

    def clear(i, carry):
        part = pl.ds(pl.multiple_of(i * TILE, TILE), TILE)
        dense[part, :] = jnp.zeros((TILE, SRC_TILES * TILE), jnp.bfloat16)
        return carry

    lax.fori_loop(0, DEST_TILES, clear, 0)
    for copy in small:
        copy.wait()
    column = lax.axis_index("col_0") * 2 + c1
    inner = lax.broadcasted_iota(jnp.int32, (TILE, PANEL), 0)
    wanted = jnp.broadcast_to(ids[...], (TILE, PANEL)) - inner
    for t in range(SRC_TILES):
        hit = wanted == (t * DEST_TILES + column) * TILE
        held[t * TILE : (t + 1) * TILE, :] = jnp.where(hit, 1.0, 0.0).astype(jnp.bfloat16)
    extra[...] = jnp.zeros((EXTRA, PANEL), jnp.float32)

    def add(k, carry):
        d, u = rows[k], cols[k]
        block = ((d & 1) ^ c1) * (DEST_TILES // 2) + (d >> 1)
        down = pl.ds(pl.multiple_of(block * TILE, TILE), TILE)
        across = pl.ds(pl.multiple_of(u * TILE, TILE), TILE)
        dense[down, across] = dense[down, across] + staged[k]
        return carry

    for n in range(KMAX // FETCH):

        @pl.when(n * FETCH < live)
        def _(n=n):
            fetch(n).wait()
            lax.fori_loop(n * FETCH, jnp.minimum(live, (n + 1) * FETCH), add, 0)

    multiply(dense.at[pl.ds(AWAY, AWAY)], held, extra, away_out)
    multiply(dense.at[pl.ds(0, AWAY)], held, extra, kept_out)


def first_products(count, rows, cols, ids, adj):
    hbm = pl.BlockSpec(memory_space=pltpu.HBM)
    chunks = jax.ShapeDtypeStruct((4, ROWS, PANEL), jnp.float32)
    dense = jax.ShapeDtypeStruct((DEST_TILES * TILE, SRC_TILES * TILE), jnp.bfloat16)
    arrays = [pltpu.with_memory_space_constraint(x, pltpu.HBM) for x in (rows, cols, ids, adj)]
    return pl.pallas_call(
        first_kernel,
        in_specs=[pl.BlockSpec(memory_space=pltpu.SMEM)] + [hbm] * 4,
        out_specs=[VMEM] * 3,
        out_shape=[chunks, chunks, dense],
        scratch_shapes=[
            pltpu.SMEM((KMAX,), jnp.int32),
            pltpu.SMEM((KMAX,), jnp.int32),
            pltpu.VMEM((1, PANEL), jnp.int32),
            pltpu.VMEM((KMAX, TILE, TILE), jnp.bfloat16),
            pltpu.VMEM((SRC_TILES * TILE, PANEL), jnp.bfloat16),
            pltpu.VMEM((EXTRA, PANEL), jnp.float32),
            pltpu.SemaphoreType.DMA((KMAX // FETCH,)),
            pltpu.SemaphoreType.DMA((3,)),
        ],
        compiler_params=WIDE,
        name="first_products",
    )(count, *arrays)


def away_kernel(dense, sources, out, held, extra):
    parts = jnp.sum(f32(sources[:, TILE:ROWS, :]), axis=0)
    squares = (parts[0:1] + parts[1:2]) + parts[2:3]
    row = lax.broadcasted_iota(jnp.int32, (EXTRA, PANEL), 0)
    extra[...] = jnp.where(row == lax.axis_index("col_1"), jnp.broadcast_to(squares, (EXTRA, PANEL)), 0.0)
    for t in range(SRC_TILES):
        held[t * TILE : (t + 1) * TILE, :] = sources[t, 0:TILE, :]
    multiply(dense.at[pl.ds(AWAY, AWAY)], held, extra, out)


def away_products(dense, sources):
    return pl.pallas_call(
        away_kernel,
        in_specs=[VMEM, VMEM],
        out_specs=[VMEM] * 3,
        out_shape=[
            jax.ShapeDtypeStruct((4, ROWS, PANEL), jnp.float32),
            jax.ShapeDtypeStruct((SRC_TILES * TILE, PANEL), jnp.bfloat16),
            jax.ShapeDtypeStruct((EXTRA, PANEL), jnp.float32),
        ],
        compiler_params=LIMIT,
        name="away_products",
    )(dense, sources)


def kept_kernel(dense, held, extra, out):
    multiply(dense.at[pl.ds(0, AWAY)], held, extra, out)


def kept_products(dense, held, extra):
    return pl.pallas_call(
        kept_kernel,
        in_specs=[VMEM] * 3,
        out_specs=VMEM,
        out_shape=jax.ShapeDtypeStruct((4, ROWS, PANEL), jnp.float32),
        compiler_params=LIMIT,
        name="kept_products",
    )(dense, held, extra)


def as_integers(x):
    x = jnp.maximum(x, 2.0**-80)
    exponent = jnp.floor(jnp.log2(x)) - 22.0
    return jnp.floor(x * jnp.exp2(-exponent) + 0.5), exponent


def encode_kernel(kept, away, *outs):
    row = lax.broadcasted_iota(jnp.int32, (EXTRA, PANEL), 0)
    for k, coded in enumerate(outs):
        chunk = (lax.axis_index("col_0") + k) & 3
        total = kept[chunk] + away[chunk]
        sums = total[0:TILE]
        lines = list(as_integers(jnp.max(sums, axis=0, keepdims=True)))
        factor = TOP / (lines[0] * jnp.exp2(lines[1]))
        codes = jnp.minimum(jnp.floor(sums * factor + 0.5), TOP).astype(jnp.int32)
        coded[0:HALF, :] = lax.shift_left(codes[0:HALF], 16) | codes[HALF:TILE]
        lines += as_integers(total[TILE : TILE + 1])
        lines += as_integers(total[TILE + 1 : TILE + 2])
        tail = jnp.zeros((EXTRA, PANEL), jnp.float32)
        for n, line in enumerate(lines):
            tail = jnp.where(row == n, jnp.broadcast_to(line, (EXTRA, PANEL)), tail)
        coded[HALF:CODED, :] = tail.astype(jnp.int32)


def encoded(kept, away):
    return pl.pallas_call(
        encode_kernel,
        in_specs=[VMEM] * 2,
        out_specs=[VMEM] * 4,
        out_shape=[jax.ShapeDtypeStruct((CODED, PANEL), jnp.int32)] * 4,
        compiler_params=LIMIT,
        name="encoded",
    )(kept, away)


def split3(x):
    high = f32(x.astype(jnp.bfloat16))
    rest = x - high
    middle = f32(rest.astype(jnp.bfloat16))
    return high, middle, rest - middle


def decoded(chunks):
    highs = jnp.zeros((HALF, PANEL), jnp.float32)
    lows = jnp.zeros((HALF, PANEL), jnp.float32)
    shares = []
    for coded in chunks:
        tail = f32(coded[HALF:CODED, :])
        power = jnp.exp2(jnp.minimum(tail, 127.0))
        step = tail[0:1] * power[1:2] * (1.0 / TOP)
        shares.append(tail[2:3] * power[3:4] + tail[4:5] * power[5:6])
        codes = coded[0:HALF, :]
        highs = highs + f32(lax.shift_right_logical(codes, 16)) * step
        lows = lows + f32(codes & 65535) * step
    return jnp.concatenate([highs, lows], axis=0), shares


def outgoing(paths, out):
    square = jnp.sum(paths * paths, axis=0, keepdims=True)
    if out.shape[0] == 1:
        out[...] = square
        return
    row = lax.broadcasted_iota(jnp.int32, (EXTRA, PANEL), 0)
    tail = jnp.zeros((EXTRA, PANEL), jnp.float32)
    for n, line in enumerate(split3(square)):
        tail = jnp.where(row == n, jnp.broadcast_to(line, (EXTRA, PANEL)), tail)
    out[0:TILE, :] = paths.astype(jnp.bfloat16)
    out[TILE:ROWS, :] = tail.astype(jnp.bfloat16)


def start_piece(ids):
    position = jnp.int32(0)
    for axis, count in zip(ROW_COL, SPLIT):
        position = position * count + lax.axis_index(axis)
    vertex = position * TILE + lax.broadcasted_iota(jnp.int32, (TILE, PANEL), 0)
    return jnp.where(vertex == jnp.broadcast_to(ids[...], (TILE, PANEL)), 1.0, 0.0)


def first_level_kernel(own, one, three, two, depth, raw, out):
    product, _ = decoded((own, one, two, three))
    paths = jnp.where(depth[...] >= 1, product, 0.0)
    raw[...] = paths
    outgoing(paths, out)


def level_kernel(level, own, one, three, two, depth, raw_in, sums_in, raw, out, sums, scale):
    before = start_piece(sums_in) if level == 2 else sums_in[...]
    product, shares = decoded((own, one, two, three))
    mean_square = jnp.zeros((1, PANEL), jnp.float32)
    for j in range(4):
        for k, share in enumerate(shares):
            here = ((lax.axis_index("col_0") - j) & 3) == k
            mean_square = mean_square + jnp.where(here, share, 0.0)
    mean_square = mean_square / VERTICES + EPSILON
    scale[...] = mean_square
    inverse = lax.rsqrt(mean_square)
    sums[...] = before + raw_in[...] * inverse
    paths = jnp.where(depth[...] >= level, product * inverse, 0.0)
    raw[...] = paths
    outgoing(paths, out)


def finish_level(level, chunks, depth, raw, sums):
    panel = jax.ShapeDtypeStruct((TILE, PANEL), jnp.float32)
    line = jax.ShapeDtypeStruct((1, PANEL), jnp.float32)
    piece = jax.ShapeDtypeStruct((ROWS, PANEL), jnp.bfloat16)
    first = level == 1
    shapes = [panel, piece if level < LEVELS else line] + ([] if first else [panel, line])
    return pl.pallas_call(
        first_level_kernel if first else lambda *refs: level_kernel(level, *refs),
        in_specs=[VMEM] * (5 if first else 7),
        out_specs=[VMEM] * len(shapes),
        out_shape=shapes,
        compiler_params=LIMIT,
        name=f"level_{level}",
    )(*chunks, depth, *(() if first else (raw, sums)))


def from_partner(x):
    return lax.ppermute(x, "col_1", [(0, 1), (1, 0)])


def along_z(x, k):
    return lax.ppermute(x, "col_0", [(i, (i + k) % 4) for i in range(4)])


def exchanged(kept, away):
    chunks = encoded(kept, from_partner(away))
    moved = {k: along_z(chunks[k], k) for k in ORDER}
    return chunks[0], moved[1], moved[3], moved[2]


def summed_alike(x, axes):
    copies = jnp.broadcast_to(x, (lax.axis_size(axes), EXTRA, PANEL))
    return jnp.sum(lax.all_to_all(copies, axes, 0, 0, tiled=True)[:, 0], axis=0, keepdims=True)


def local(adj_tiles, tile_rows, tile_cols, tile_count, tile_depth, source_ids):
    away, kept, dense = first_products(
        tile_count, tile_rows[0, 0], tile_cols[0, 0], source_ids[None, :], adj_tiles[0, 0]
    )
    sums = source_ids[None, :]
    raw, piece, *_ = finish_level(1, exchanged(kept, away), tile_depth, None, None)
    scales = []
    for level in range(2, LEVELS + 1):
        spread = jnp.broadcast_to(piece, (SRC_TILES, ROWS, PANEL))
        sources = lax.all_to_all(spread, ROW, 0, 0, tiled=True)
        away, held, extra = away_products(dense, sources)
        chunks = exchanged(kept_products(dense, held, extra), away)
        raw, piece, sums, scale = finish_level(level, chunks, tile_depth, raw, sums)
        scales.append(scale)
    squares = piece
    total = summed_alike(summed_alike(squares, ("row_1",) + COL), ("row_0", "row_2"))
    mean_square = total / VERTICES + EPSILON
    scales.append(mean_square)
    path_sums = sums + raw * lax.rsqrt(mean_square)
    return path_sums, 0.5 * jnp.log(jnp.concatenate(scales, axis=0))


def solution(mesh):
    split = Mesh(mesh.devices.reshape(SPLIT), ROW_COL)
    in_specs = (
        P(ROW, COL, None, None, None),
        P(ROW, COL, None),
        P(ROW, COL, None),
        P(ROW, COL),
        P(ROW_COL, None),
        P(),
    )
    out_specs = (P(ROW_COL, None), P())
    return jax.shard_map(local, mesh=split, in_specs=in_specs, out_specs=out_specs, check_vma=False)
```

```python
import jax
import jax.numpy as jnp
from jax import lax
from jax.experimental import pallas as pl
from jax.experimental.pallas import tpu as pltpu
from jax.sharding import Mesh
from jax.sharding import PartitionSpec as P

TILE = 128
PANEL = 128
LEVELS = 6
KMAX = 128
DEST_TILES = 8
SRC_TILES = 32
VERTICES = 32768
EPSILON = 1e-06
ROW = ("row_0", "row_1", "row_2")
COL = ("col_0", "col_1")
ROW_COL = ROW + COL
SPLIT = (4, 2, 4, 4, 2)
HALF = TILE // 2
EXTRA = 8
ROWS = TILE + EXTRA
CODED = HALF + EXTRA
AWAY = DEST_TILES // 2 * TILE
TOP = 65535.0
ORDER = (2, 1, 3)
FETCH = 16
TOGETHER = 8
VMEM = pl.BlockSpec(memory_space=pltpu.VMEM)
WIDE = pltpu.CompilerParams(vmem_limit_bytes=16 * 1024 * 1024)
LIMIT = pltpu.CompilerParams(vmem_limit_bytes=4 * 1024 * 1024)


def f32(x):
    return x.astype(jnp.float32)


def multiply(dense, held, extra, out):
    product = jnp.dot(dense[...], held[...], preferred_element_type=jnp.float32)
    for k in range(4):
        out[k, 0:TILE, :] = product[k * TILE : (k + 1) * TILE]
        out[k, TILE:ROWS, :] = extra[...]


def first_kernel(
    count, rows_in, cols_in, ids_in, adj, away_out, kept_out, dense,
    rows, cols, ids, staged, held, extra, sems, stores,
):
    c1 = lax.axis_index("col_1")

    def fetch(n):
        part = pl.ds(n * FETCH, FETCH)
        return pltpu.make_async_copy(adj.at[part], staged.at[part], sems.at[n])

    small = [
        pltpu.make_async_copy(source, target, stores.at[i])
        for i, (source, target) in enumerate(((ids_in, ids), (rows_in, rows), (cols_in, cols)))
    ]
    for copy in small:
        copy.start()
    live = count[0, 0]
    for n in range(KMAX // FETCH):

        @pl.when(n * FETCH < live)
        def _(n=n):
            fetch(n).start()

    def clear(i, carry):
        part = pl.ds(pl.multiple_of(i * TILE, TILE), TILE)
        dense[part, :] = jnp.zeros((TILE, SRC_TILES * TILE), jnp.bfloat16)
        return carry

    lax.fori_loop(0, DEST_TILES, clear, 0)
    for copy in small:
        copy.wait()
    column = lax.axis_index("col_0") * 2 + c1
    inner = lax.broadcasted_iota(jnp.int32, (TILE, PANEL), 0)
    wanted = jnp.broadcast_to(ids[...], (TILE, PANEL)) - inner
    for t in range(SRC_TILES):
        hit = wanted == (t * DEST_TILES + column) * TILE
        held[t * TILE : (t + 1) * TILE, :] = jnp.where(hit, 1.0, 0.0).astype(jnp.bfloat16)
    extra[...] = jnp.zeros((EXTRA, PANEL), jnp.float32)

    def add(k):
        d, u = rows[k], cols[k]
        block = ((d & 1) ^ c1) * (DEST_TILES // 2) + (d >> 1)
        down = pl.ds(pl.multiple_of(block * TILE, TILE), TILE)
        across = pl.ds(pl.multiple_of(u * TILE, TILE), TILE)
        dense[down, across] = dense[down, across] + staged[k]

    def add_some(g, carry):
        for i in range(TOGETHER):
            add(g * TOGETHER + i)
        return carry

    def add_one(k, carry):
        add(k)
        return carry

    whole = live // TOGETHER
    for n in range(KMAX // FETCH):

        @pl.when(n * FETCH < live)
        def _(n=n):
            fetch(n).wait()
            step = FETCH // TOGETHER
            lax.fori_loop(n * step, jnp.minimum(whole, (n + 1) * step), add_some, 0)

    lax.fori_loop(whole * TOGETHER, live, add_one, 0)
    multiply(dense.at[pl.ds(AWAY, AWAY)], held, extra, away_out)
    multiply(dense.at[pl.ds(0, AWAY)], held, extra, kept_out)


def first_products(count, rows, cols, ids, adj):
    hbm = pl.BlockSpec(memory_space=pltpu.HBM)
    chunks = jax.ShapeDtypeStruct((4, ROWS, PANEL), jnp.float32)
    dense = jax.ShapeDtypeStruct((DEST_TILES * TILE, SRC_TILES * TILE), jnp.bfloat16)
    arrays = [pltpu.with_memory_space_constraint(x, pltpu.HBM) for x in (rows, cols, ids, adj)]
    return pl.pallas_call(
        first_kernel,
        in_specs=[pl.BlockSpec(memory_space=pltpu.SMEM)] + [hbm] * 4,
        out_specs=[VMEM] * 3,
        out_shape=[chunks, chunks, dense],
        scratch_shapes=[
            pltpu.SMEM((KMAX,), jnp.int32),
            pltpu.SMEM((KMAX,), jnp.int32),
            pltpu.VMEM((1, PANEL), jnp.int32),
            pltpu.VMEM((KMAX, TILE, TILE), jnp.bfloat16),
            pltpu.VMEM((SRC_TILES * TILE, PANEL), jnp.bfloat16),
            pltpu.VMEM((EXTRA, PANEL), jnp.float32),
            pltpu.SemaphoreType.DMA((KMAX // FETCH,)),
            pltpu.SemaphoreType.DMA((3,)),
        ],
        compiler_params=WIDE,
        name="first_products",
    )(count, *arrays)


def away_kernel(dense, sources, out, held, extra):
    parts = jnp.sum(f32(sources[:, TILE:ROWS, :]), axis=0)
    squares = (parts[0:1] + parts[1:2]) + parts[2:3]
    row = lax.broadcasted_iota(jnp.int32, (EXTRA, PANEL), 0)
    extra[...] = jnp.where(row == lax.axis_index("col_1"), jnp.broadcast_to(squares, (EXTRA, PANEL)), 0.0)
    for t in range(SRC_TILES):
        held[t * TILE : (t + 1) * TILE, :] = sources[t, 0:TILE, :]
    multiply(dense.at[pl.ds(AWAY, AWAY)], held, extra, out)


def away_products(dense, sources):
    return pl.pallas_call(
        away_kernel,
        in_specs=[VMEM, VMEM],
        out_specs=[VMEM] * 3,
        out_shape=[
            jax.ShapeDtypeStruct((4, ROWS, PANEL), jnp.float32),
            jax.ShapeDtypeStruct((SRC_TILES * TILE, PANEL), jnp.bfloat16),
            jax.ShapeDtypeStruct((EXTRA, PANEL), jnp.float32),
        ],
        compiler_params=LIMIT,
        name="away_products",
    )(dense, sources)


def kept_kernel(dense, held, extra, out):
    multiply(dense.at[pl.ds(0, AWAY)], held, extra, out)


def kept_products(dense, held, extra):
    return pl.pallas_call(
        kept_kernel,
        in_specs=[VMEM] * 3,
        out_specs=VMEM,
        out_shape=jax.ShapeDtypeStruct((4, ROWS, PANEL), jnp.float32),
        compiler_params=LIMIT,
        name="kept_products",
    )(dense, held, extra)


def as_integers(x):
    x = jnp.maximum(x, 2.0**-80)
    exponent = jnp.floor(jnp.log2(x)) - 22.0
    return jnp.floor(x * jnp.exp2(-exponent) + 0.5), exponent


def encode_kernel(kept, away, *outs):
    row = lax.broadcasted_iota(jnp.int32, (EXTRA, PANEL), 0)
    for k, coded in enumerate(outs):
        chunk = (lax.axis_index("col_0") + k) & 3
        total = kept[chunk] + away[chunk]
        sums = total[0:TILE]
        lines = list(as_integers(jnp.max(sums, axis=0, keepdims=True)))
        factor = TOP / jnp.sqrt(jnp.sqrt(lines[0] * jnp.exp2(lines[1])))
        codes = jnp.floor(jnp.sqrt(jnp.sqrt(sums)) * factor + 0.5)
        codes = jnp.minimum(codes, TOP).astype(jnp.int32)
        coded[0:HALF, :] = lax.shift_left(codes[0:HALF], 16) | codes[HALF:TILE]
        lines += as_integers(total[TILE : TILE + 1])
        lines += as_integers(total[TILE + 1 : TILE + 2])
        tail = jnp.zeros((EXTRA, PANEL), jnp.float32)
        for n, line in enumerate(lines):
            tail = jnp.where(row == n, jnp.broadcast_to(line, (EXTRA, PANEL)), tail)
        coded[HALF:CODED, :] = tail.astype(jnp.int32)


def encoded(kept, away):
    return pl.pallas_call(
        encode_kernel,
        in_specs=[VMEM] * 2,
        out_specs=[VMEM] * 4,
        out_shape=[jax.ShapeDtypeStruct((CODED, PANEL), jnp.int32)] * 4,
        compiler_params=LIMIT,
        name="encoded",
    )(kept, away)


def split3(x):
    high = f32(x.astype(jnp.bfloat16))
    rest = x - high
    middle = f32(rest.astype(jnp.bfloat16))
    return high, middle, rest - middle


def fourth_power(codes):
    root = f32(codes) * (1.0 / TOP)
    return (root * root) * (root * root)


def decoded(chunks):
    highs = jnp.zeros((HALF, PANEL), jnp.float32)
    lows = jnp.zeros((HALF, PANEL), jnp.float32)
    shares = []
    for coded in chunks:
        tail = f32(coded[HALF:CODED, :])
        power = jnp.exp2(jnp.minimum(tail, 127.0))
        scale = tail[0:1] * power[1:2]
        shares.append(tail[2:3] * power[3:4] + tail[4:5] * power[5:6])
        codes = coded[0:HALF, :]
        highs = highs + fourth_power(lax.shift_right_logical(codes, 16)) * scale
        lows = lows + fourth_power(codes & 65535) * scale
    return jnp.concatenate([highs, lows], axis=0), shares


def outgoing(paths, out):
    square = jnp.sum(paths * paths, axis=0, keepdims=True)
    if out.shape[0] == 1:
        out[...] = square
        return
    row = lax.broadcasted_iota(jnp.int32, (EXTRA, PANEL), 0)
    tail = jnp.zeros((EXTRA, PANEL), jnp.float32)
    for n, line in enumerate(split3(square)):
        tail = jnp.where(row == n, jnp.broadcast_to(line, (EXTRA, PANEL)), tail)
    out[0:TILE, :] = paths.astype(jnp.bfloat16)
    out[TILE:ROWS, :] = tail.astype(jnp.bfloat16)


def start_piece(ids):
    position = jnp.int32(0)
    for axis, count in zip(ROW_COL, SPLIT):
        position = position * count + lax.axis_index(axis)
    vertex = position * TILE + lax.broadcasted_iota(jnp.int32, (TILE, PANEL), 0)
    return jnp.where(vertex == jnp.broadcast_to(ids[...], (TILE, PANEL)), 1.0, 0.0)


def first_level_kernel(own, two, one, three, depth, raw, out):
    product, _ = decoded((own, one, two, three))
    paths = jnp.where(depth[...] >= 1, product, 0.0)
    raw[...] = paths
    outgoing(paths, out)


def level_kernel(level, own, two, one, three, depth, raw_in, sums_in, raw, out, sums, scale):
    before = start_piece(sums_in) if level == 2 else sums_in[...]
    product, shares = decoded((own, one, two, three))
    mean_square = jnp.zeros((1, PANEL), jnp.float32)
    for j in range(4):
        for k, share in enumerate(shares):
            here = ((lax.axis_index("col_0") - j) & 3) == k
            mean_square = mean_square + jnp.where(here, share, 0.0)
    mean_square = mean_square / VERTICES + EPSILON
    scale[...] = mean_square
    inverse = lax.rsqrt(mean_square)
    sums[...] = before + raw_in[...] * inverse
    paths = jnp.where(depth[...] >= level, product * inverse, 0.0)
    raw[...] = paths
    outgoing(paths, out)


def finish_level(level, chunks, depth, raw, sums):
    panel = jax.ShapeDtypeStruct((TILE, PANEL), jnp.float32)
    line = jax.ShapeDtypeStruct((1, PANEL), jnp.float32)
    piece = jax.ShapeDtypeStruct((ROWS, PANEL), jnp.bfloat16)
    first = level == 1
    shapes = [panel, piece if level < LEVELS else line] + ([] if first else [panel, line])
    return pl.pallas_call(
        first_level_kernel if first else lambda *refs: level_kernel(level, *refs),
        in_specs=[VMEM] * (5 if first else 7),
        out_specs=[VMEM] * len(shapes),
        out_shape=shapes,
        compiler_params=LIMIT,
        name=f"level_{level}",
    )(*chunks, depth, *(() if first else (raw, sums)))


def from_partner(x):
    return lax.ppermute(x, "col_1", [(0, 1), (1, 0)])


def along_z(x, k):
    return lax.ppermute(x, "col_0", [(i, (i + k) % 4) for i in range(4)])


def exchanged(kept, away):
    chunks = encoded(kept, from_partner(away))
    moved = {k: along_z(chunks[k], k) for k in ORDER}
    return (chunks[0], *(moved[k] for k in ORDER))


def everywhere(line, axes):
    copies = jnp.broadcast_to(line, (lax.axis_size(axes), EXTRA, PANEL))
    return lax.all_to_all(copies, axes, 0, 0, tiled=True)


def last_kernel(squares, raw, sums, *refs):
    scales, (path_sums, log_scales) = refs[:-2], refs[-2:]
    total = squares[0, 0:1, :]
    for i in range(1, squares.shape[0]):
        total = total + squares[i, 0:1, :]
    mean_square = total / VERTICES + EPSILON
    path_sums[...] = sums[...] + raw[...] * lax.rsqrt(mean_square)
    for n, scale in enumerate(scales):
        log_scales[n : n + 1, :] = 0.5 * jnp.log(scale[...])
    log_scales[LEVELS - 1 : LEVELS, :] = 0.5 * jnp.log(mean_square)


def last_level(squares, raw, sums, scales):
    return pl.pallas_call(
        last_kernel,
        in_specs=[VMEM] * (3 + len(scales)),
        out_specs=[VMEM] * 2,
        out_shape=[
            jax.ShapeDtypeStruct((TILE, PANEL), jnp.float32),
            jax.ShapeDtypeStruct((LEVELS, PANEL), jnp.float32),
        ],
        compiler_params=LIMIT,
        name="last_level",
    )(squares, raw, sums, *scales)


def local(adj_tiles, tile_rows, tile_cols, tile_count, tile_depth, source_ids):
    away, kept, dense = first_products(
        tile_count, tile_rows[0, 0], tile_cols[0, 0], source_ids[None, :], adj_tiles[0, 0]
    )
    sums = source_ids[None, :]
    raw, piece, *_ = finish_level(1, exchanged(kept, away), tile_depth, None, None)
    scales = []
    for level in range(2, LEVELS + 1):
        spread = jnp.broadcast_to(piece, (SRC_TILES, ROWS, PANEL))
        sources = lax.all_to_all(spread, ROW, 0, 0, tiled=True)
        away, held, extra = away_products(dense, sources)
        chunks = exchanged(kept_products(dense, held, extra), away)
        raw, piece, sums, scale = finish_level(level, chunks, tile_depth, raw, sums)
        scales.append(scale)
    squares = jnp.sum(everywhere(piece, ("row_1",) + COL)[:, 0], axis=0, keepdims=True)
    return tuple(last_level(everywhere(squares, ("row_0", "row_2")), raw, sums, scales))


def solution(mesh):
    split = Mesh(mesh.devices.reshape(SPLIT), ROW_COL)
    in_specs = (
        P(ROW, COL, None, None, None),
        P(ROW, COL, None),
        P(ROW, COL, None),
        P(ROW, COL),
        P(ROW_COL, None),
        P(),
    )
    out_specs = (P(ROW_COL, None), P())
    return jax.shard_map(local, mesh=split, in_specs=in_specs, out_specs=out_specs, check_vma=False)
```

```python
import jax
import jax.numpy as jnp
from jax import lax
from jax.experimental import pallas as pl
from jax.experimental.pallas import tpu as pltpu
from jax.sharding import Mesh
from jax.sharding import PartitionSpec as P

TILE = 128
PANEL = 128
LEVELS = 6
KMAX = 128
DEST_TILES = 8
SRC_TILES = 32
VERTICES = 32768
EPSILON = 1e-06
ROW = ("row_0", "row_1", "row_2")
COL = ("col_0", "col_1")
ROW_COL = ROW + COL
SPLIT = (4, 2, 4, 4, 2)
HALF = TILE // 2
EXTRA = 8
ROWS = TILE + EXTRA
CODED = HALF + EXTRA
AWAY = DEST_TILES // 2 * TILE
TOP = 65535.0
FETCH = 16
TOGETHER = 8
VMEM = pl.BlockSpec(memory_space=pltpu.VMEM)
WIDE = pltpu.CompilerParams(vmem_limit_bytes=16 * 1024 * 1024)
LIMIT = pltpu.CompilerParams(vmem_limit_bytes=4 * 1024 * 1024)


def f32(x):
    return x.astype(jnp.float32)


def multiply(dense, held, extra, out):
    product = jnp.dot(dense[...], held[...], preferred_element_type=jnp.float32)
    for k in range(4):
        out[k, 0:TILE, :] = product[k * TILE : (k + 1) * TILE]
        out[k, TILE:ROWS, :] = extra[...]


def first_kernel(
    count, rows_in, cols_in, ids_in, adj, away_out, kept_out, dense,
    rows, cols, ids, staged, held, extra, sems, stores,
):
    c1 = lax.axis_index("col_1")

    def fetch(n):
        part = pl.ds(n * FETCH, FETCH)
        return pltpu.make_async_copy(adj.at[part], staged.at[part], sems.at[n])

    small = [
        pltpu.make_async_copy(source, target, stores.at[i])
        for i, (source, target) in enumerate(((ids_in, ids), (rows_in, rows), (cols_in, cols)))
    ]
    for copy in small:
        copy.start()
    live = count[0, 0]
    for n in range(KMAX // FETCH):

        @pl.when(n * FETCH < live)
        def _(n=n):
            fetch(n).start()

    def clear(i, carry):
        part = pl.ds(pl.multiple_of(i * TILE, TILE), TILE)
        dense[part, :] = jnp.zeros((TILE, SRC_TILES * TILE), jnp.bfloat16)
        return carry

    lax.fori_loop(0, DEST_TILES, clear, 0)
    for copy in small:
        copy.wait()
    c0 = lax.axis_index("col_0")
    column = c0 * 2 + c1
    inner = lax.broadcasted_iota(jnp.int32, (TILE, PANEL), 0)
    wanted = jnp.broadcast_to(ids[...], (TILE, PANEL)) - inner
    for t in range(SRC_TILES):
        hit = wanted == (t * DEST_TILES + column) * TILE
        held[t * TILE : (t + 1) * TILE, :] = jnp.where(hit, 1.0, 0.0).astype(jnp.bfloat16)
    extra[...] = jnp.zeros((EXTRA, PANEL), jnp.float32)

    def add(k):
        d, u = rows[k], cols[k]
        step = ((d >> 1) - c0) & 3
        beside = (step & 1) == 1
        owner = jnp.where(beside, step >> 1, d & 1)
        spot = jnp.where(beside, (d & 1) ^ owner, 3 - (step >> 1))
        block = (owner ^ c1) * (DEST_TILES // 2) + spot
        down = pl.ds(pl.multiple_of(block * TILE, TILE), TILE)
        across = pl.ds(pl.multiple_of(u * TILE, TILE), TILE)
        dense[down, across] = dense[down, across] + staged[k]

    def add_some(g, carry):
        for i in range(TOGETHER):
            add(g * TOGETHER + i)
        return carry

    def add_one(k, carry):
        add(k)
        return carry

    whole = live // TOGETHER
    for n in range(KMAX // FETCH):

        @pl.when(n * FETCH < live)
        def _(n=n):
            fetch(n).wait()
            step = FETCH // TOGETHER
            lax.fori_loop(n * step, jnp.minimum(whole, (n + 1) * step), add_some, 0)

    lax.fori_loop(whole * TOGETHER, live, add_one, 0)
    multiply(dense.at[pl.ds(AWAY, AWAY)], held, extra, away_out)
    multiply(dense.at[pl.ds(0, AWAY)], held, extra, kept_out)


def first_products(count, rows, cols, ids, adj):
    hbm = pl.BlockSpec(memory_space=pltpu.HBM)
    chunks = jax.ShapeDtypeStruct((4, ROWS, PANEL), jnp.float32)
    dense = jax.ShapeDtypeStruct((DEST_TILES * TILE, SRC_TILES * TILE), jnp.bfloat16)
    arrays = [pltpu.with_memory_space_constraint(x, pltpu.HBM) for x in (rows, cols, ids, adj)]
    return pl.pallas_call(
        first_kernel,
        in_specs=[pl.BlockSpec(memory_space=pltpu.SMEM)] + [hbm] * 4,
        out_specs=[VMEM] * 3,
        out_shape=[chunks, chunks, dense],
        scratch_shapes=[
            pltpu.SMEM((KMAX,), jnp.int32),
            pltpu.SMEM((KMAX,), jnp.int32),
            pltpu.VMEM((1, PANEL), jnp.int32),
            pltpu.VMEM((KMAX, TILE, TILE), jnp.bfloat16),
            pltpu.VMEM((SRC_TILES * TILE, PANEL), jnp.bfloat16),
            pltpu.VMEM((EXTRA, PANEL), jnp.float32),
            pltpu.SemaphoreType.DMA((KMAX // FETCH,)),
            pltpu.SemaphoreType.DMA((3,)),
        ],
        compiler_params=WIDE,
        name="first_products",
    )(count, *arrays)


def away_kernel(dense, sources, out, held, extra):
    parts = jnp.sum(f32(sources[:, TILE:ROWS, :]), axis=0)
    squares = (parts[0:1] + parts[1:2]) + parts[2:3]
    row = lax.broadcasted_iota(jnp.int32, (EXTRA, PANEL), 0)
    extra[...] = jnp.where(row == lax.axis_index("col_1"), jnp.broadcast_to(squares, (EXTRA, PANEL)), 0.0)
    for t in range(SRC_TILES):
        held[t * TILE : (t + 1) * TILE, :] = sources[t, 0:TILE, :]
    multiply(dense.at[pl.ds(AWAY, AWAY)], held, extra, out)


def away_products(dense, sources):
    return pl.pallas_call(
        away_kernel,
        in_specs=[VMEM, VMEM],
        out_specs=[VMEM] * 3,
        out_shape=[
            jax.ShapeDtypeStruct((4, ROWS, PANEL), jnp.float32),
            jax.ShapeDtypeStruct((SRC_TILES * TILE, PANEL), jnp.bfloat16),
            jax.ShapeDtypeStruct((EXTRA, PANEL), jnp.float32),
        ],
        compiler_params=LIMIT,
        name="away_products",
    )(dense, sources)


def kept_kernel(dense, held, extra, out):
    multiply(dense.at[pl.ds(0, AWAY)], held, extra, out)


def kept_products(dense, held, extra):
    return pl.pallas_call(
        kept_kernel,
        in_specs=[VMEM] * 3,
        out_specs=VMEM,
        out_shape=jax.ShapeDtypeStruct((4, ROWS, PANEL), jnp.float32),
        compiler_params=LIMIT,
        name="kept_products",
    )(dense, held, extra)


def as_integers(x):
    x = jnp.maximum(x, 2.0**-80)
    exponent = jnp.floor(jnp.log2(x)) - 22.0
    return jnp.floor(x * jnp.exp2(-exponent) + 0.5), exponent


def encode_kernel(kept, away, beside, far, own):
    row = lax.broadcasted_iota(jnp.int32, (EXTRA, PANEL), 0)
    for k, coded in enumerate((beside.at[0], beside.at[1], far, own)):
        total = kept[k] + away[k]
        sums = total[0:TILE]
        lines = list(as_integers(jnp.max(sums, axis=0, keepdims=True)))
        factor = TOP / jnp.sqrt(jnp.sqrt(lines[0] * jnp.exp2(lines[1])))
        codes = jnp.floor(jnp.sqrt(jnp.sqrt(sums)) * factor + 0.5)
        codes = jnp.minimum(codes, TOP).astype(jnp.int32)
        coded[0:HALF, :] = lax.shift_left(codes[0:HALF], 16) | codes[HALF:TILE]
        lines += as_integers(total[TILE : TILE + 1])
        lines += as_integers(total[TILE + 1 : TILE + 2])
        tail = jnp.zeros((EXTRA, PANEL), jnp.float32)
        for n, line in enumerate(lines):
            tail = jnp.where(row == n, jnp.broadcast_to(line, (EXTRA, PANEL)), tail)
        coded[HALF:CODED, :] = tail.astype(jnp.int32)


def encoded(kept, away):
    return pl.pallas_call(
        encode_kernel,
        in_specs=[VMEM] * 2,
        out_specs=[VMEM] * 3,
        out_shape=[
            jax.ShapeDtypeStruct((2, CODED, PANEL), jnp.int32),
            jax.ShapeDtypeStruct((CODED, PANEL), jnp.int32),
            jax.ShapeDtypeStruct((CODED, PANEL), jnp.int32),
        ],
        compiler_params=LIMIT,
        name="encoded",
    )(kept, away)


def split3(x):
    high = f32(x.astype(jnp.bfloat16))
    rest = x - high
    middle = f32(rest.astype(jnp.bfloat16))
    return high, middle, rest - middle


def fourth_power(codes):
    root = f32(codes) * (1.0 / TOP)
    return (root * root) * (root * root)


def decoded(chunks):
    highs = jnp.zeros((HALF, PANEL), jnp.float32)
    lows = jnp.zeros((HALF, PANEL), jnp.float32)
    shares = []
    for coded in chunks:
        tail = f32(coded[HALF:CODED, :])
        power = jnp.exp2(jnp.minimum(tail, 127.0))
        scale = tail[0:1] * power[1:2]
        shares.append(tail[2:3] * power[3:4] + tail[4:5] * power[5:6])
        codes = coded[0:HALF, :]
        highs = highs + fourth_power(lax.shift_right_logical(codes, 16)) * scale
        lows = lows + fourth_power(codes & 65535) * scale
    return jnp.concatenate([highs, lows], axis=0), shares


def outgoing(paths, out):
    square = jnp.sum(paths * paths, axis=0, keepdims=True)
    if out.shape[0] == 1:
        out[...] = square
        return
    row = lax.broadcasted_iota(jnp.int32, (EXTRA, PANEL), 0)
    tail = jnp.zeros((EXTRA, PANEL), jnp.float32)
    for n, line in enumerate(split3(square)):
        tail = jnp.where(row == n, jnp.broadcast_to(line, (EXTRA, PANEL)), tail)
    out[0:TILE, :] = paths.astype(jnp.bfloat16)
    out[TILE:ROWS, :] = tail.astype(jnp.bfloat16)


def start_piece(ids):
    position = jnp.int32(0)
    for axis, count in zip(ROW_COL, SPLIT):
        position = position * count + lax.axis_index(axis)
    vertex = position * TILE + lax.broadcasted_iota(jnp.int32, (TILE, PANEL), 0)
    return jnp.where(vertex == jnp.broadcast_to(ids[...], (TILE, PANEL)), 1.0, 0.0)


def first_level_kernel(own, heard, handed, far, depth, raw, out):
    product, _ = decoded((own, heard.at[0], handed, far))
    paths = jnp.where(depth[...] >= 1, product, 0.0)
    raw[...] = paths
    outgoing(paths, out)


def level_kernel(level, own, heard, handed, far, depth, raw_in, sums_in, raw, out, sums, scale):
    before = start_piece(sums_in) if level == 2 else sums_in[...]
    product, shares = decoded((own, heard.at[0], handed, far))
    mean_square = jnp.zeros((1, PANEL), jnp.float32)
    turned = 2 * lax.axis_index("col_1")
    back = (0, 1 + turned, 3 - turned, 2)
    for j in range(4):
        for k, share in zip(back, shares):
            here = ((lax.axis_index("col_0") - j) & 3) == k
            mean_square = mean_square + jnp.where(here, share, 0.0)
    mean_square = mean_square / VERTICES + EPSILON
    scale[...] = mean_square
    inverse = lax.rsqrt(mean_square)
    sums[...] = before + raw_in[...] * inverse
    paths = jnp.where(depth[...] >= level, product * inverse, 0.0)
    raw[...] = paths
    outgoing(paths, out)


def finish_level(level, chunks, depth, raw, sums):
    panel = jax.ShapeDtypeStruct((TILE, PANEL), jnp.float32)
    line = jax.ShapeDtypeStruct((1, PANEL), jnp.float32)
    piece = jax.ShapeDtypeStruct((ROWS, PANEL), jnp.bfloat16)
    first = level == 1
    shapes = [panel, piece if level < LEVELS else line] + ([] if first else [panel, line])
    return pl.pallas_call(
        first_level_kernel if first else lambda *refs: level_kernel(level, *refs),
        in_specs=[VMEM] * (5 if first else 7),
        out_specs=[VMEM] * len(shapes),
        out_shape=shapes,
        compiler_params=LIMIT,
        name=f"level_{level}",
    )(*chunks, depth, *(() if first else (raw, sums)))


def from_partner(x):
    return lax.ppermute(x, "col_1", [(0, 1), (1, 0)])


def exchanged(kept, away):
    beside, far, own = encoded(kept, from_partner(away))
    forward = [(2 * i, 2 * ((i + 1) % 4)) for i in range(4)]
    backward = [(2 * i + 1, 2 * ((i - 1) % 4) + 1) for i in range(4)]
    heard = lax.ppermute(beside, COL, forward + backward)
    handed = from_partner(heard[1])
    far = lax.ppermute(far, "col_0", [(i, (i + 2) % 4) for i in range(4)])
    return own, heard, handed, far


def everywhere(line, axes):
    copies = jnp.broadcast_to(line, (lax.axis_size(axes), EXTRA, PANEL))
    return lax.all_to_all(copies, axes, 0, 0, tiled=True)


def last_kernel(squares, raw, sums, *refs):
    scales, (path_sums, log_scales) = refs[:-2], refs[-2:]
    total = squares[0, 0:1, :]
    for i in range(1, squares.shape[0]):
        total = total + squares[i, 0:1, :]
    mean_square = total / VERTICES + EPSILON
    path_sums[...] = sums[...] + raw[...] * lax.rsqrt(mean_square)
    for n, scale in enumerate(scales):
        log_scales[n : n + 1, :] = 0.5 * jnp.log(scale[...])
    log_scales[LEVELS - 1 : LEVELS, :] = 0.5 * jnp.log(mean_square)


def last_level(squares, raw, sums, scales):
    return pl.pallas_call(
        last_kernel,
        in_specs=[VMEM] * (3 + len(scales)),
        out_specs=[VMEM] * 2,
        out_shape=[
            jax.ShapeDtypeStruct((TILE, PANEL), jnp.float32),
            jax.ShapeDtypeStruct((LEVELS, PANEL), jnp.float32),
        ],
        compiler_params=LIMIT,
        name="last_level",
    )(squares, raw, sums, *scales)


def local(adj_tiles, tile_rows, tile_cols, tile_count, tile_depth, source_ids):
    away, kept, dense = first_products(
        tile_count, tile_rows[0, 0], tile_cols[0, 0], source_ids[None, :], adj_tiles[0, 0]
    )
    sums = source_ids[None, :]
    raw, piece, *_ = finish_level(1, exchanged(kept, away), tile_depth, None, None)
    scales = []
    for level in range(2, LEVELS + 1):
        spread = jnp.broadcast_to(piece, (SRC_TILES, ROWS, PANEL))
        sources = lax.all_to_all(spread, ROW, 0, 0, tiled=True)
        away, held, extra = away_products(dense, sources)
        chunks = exchanged(kept_products(dense, held, extra), away)
        raw, piece, sums, scale = finish_level(level, chunks, tile_depth, raw, sums)
        scales.append(scale)
    squares = jnp.sum(everywhere(piece, ("row_1",) + COL)[:, 0], axis=0, keepdims=True)
    return tuple(last_level(everywhere(squares, ("row_0", "row_2")), raw, sums, scales))


def solution(mesh):
    split = Mesh(mesh.devices.reshape(SPLIT), ROW_COL)
    in_specs = (
        P(ROW, COL, None, None, None),
        P(ROW, COL, None),
        P(ROW, COL, None),
        P(ROW, COL),
        P(ROW_COL, None),
        P(),
    )
    out_specs = (P(ROW_COL, None), P())
    return jax.shard_map(local, mesh=split, in_specs=in_specs, out_specs=out_specs, check_vma=False)
```

```python
import jax
import jax.numpy as jnp
from jax import lax
from jax.experimental import pallas as pl
from jax.experimental.pallas import tpu as pltpu
from jax.sharding import Mesh
from jax.sharding import PartitionSpec as P


TILE = 128
PANEL = 128
LEVELS = 6
KMAX = 128
DEST_TILES = 8
SRC_TILES = 32
VERTICES = 32768
EPSILON = 1e-06
ROW = ("row_0", "row_1", "row_2")
COL = ("col_0", "col_1")
ROW_COL = ROW + COL
SPLIT = (4, 2, 4, 4, 2)
HALF = TILE // 2
EXTRA = 8
ROWS = TILE + EXTRA
CODED = HALF + EXTRA
AWAY = DEST_TILES // 2 * TILE
TOP = 65535.0
FETCH = 16
TOGETHER = 8
VMEM = pl.BlockSpec(memory_space=pltpu.VMEM)
WIDE = pltpu.CompilerParams(vmem_limit_bytes=16 * 1024 * 1024)
LIMIT = pltpu.CompilerParams(vmem_limit_bytes=4 * 1024 * 1024)


def f32(x):
    return x.astype(jnp.float32)


def multiply(dense, held, extra, out):
    product = jnp.dot(dense[...], held[...], preferred_element_type=jnp.float32)
    for k in range(4):
        out[k, 0:TILE, :] = product[k * TILE : (k + 1) * TILE]
        out[k, TILE:ROWS, :] = extra[...]


def first_kernel(
    count, rows_in, cols_in, ids_in, adj, away_out, kept_out, dense,
    rows, cols, ids, staged, held, extra, sems, stores,
):
    c1 = lax.axis_index("col_1")

    def fetch(n):
        part = pl.ds(n * FETCH, FETCH)
        return pltpu.make_async_copy(adj.at[part], staged.at[part], sems.at[n])

    small = [
        pltpu.make_async_copy(source, target, stores.at[i])
        for i, (source, target) in enumerate(((ids_in, ids), (rows_in, rows), (cols_in, cols)))
    ]
    for copy in small:
        copy.start()
    live = count[0, 0]
    for n in range(KMAX // FETCH):

        @pl.when(n * FETCH < live)
        def _(n=n):
            fetch(n).start()

    def clear(i, carry):
        part = pl.ds(pl.multiple_of(i * TILE, TILE), TILE)
        dense[part, :] = jnp.zeros((TILE, SRC_TILES * TILE), jnp.bfloat16)
        return carry

    lax.fori_loop(0, DEST_TILES, clear, 0)
    for copy in small:
        copy.wait()
    c0 = lax.axis_index("col_0")
    column = c0 * 2 + c1
    inner = lax.broadcasted_iota(jnp.int32, (TILE, PANEL), 0)
    wanted = jnp.broadcast_to(ids[...], (TILE, PANEL)) - inner
    for t in range(SRC_TILES):
        hit = wanted == (t * DEST_TILES + column) * TILE
        held[t * TILE : (t + 1) * TILE, :] = jnp.where(hit, 1.0, 0.0).astype(jnp.bfloat16)
    extra[...] = jnp.zeros((EXTRA, PANEL), jnp.float32)

    def add(k):
        d, u = rows[k], cols[k]
        step = ((d >> 1) - c0) & 3
        beside = (step & 1) == 1
        owner = jnp.where(beside, step >> 1, d & 1)
        spot = jnp.where(beside, (d & 1) ^ owner, 3 - (step >> 1))
        block = (owner ^ c1) * (DEST_TILES // 2) + spot
        down = pl.ds(pl.multiple_of(block * TILE, TILE), TILE)
        across = pl.ds(pl.multiple_of(u * TILE, TILE), TILE)
        dense[down, across] = dense[down, across] + staged[k]

    def add_some(g, carry):
        for i in range(TOGETHER):
            add(g * TOGETHER + i)
        return carry

    def add_one(k, carry):
        add(k)
        return carry

    whole = live // TOGETHER
    for n in range(KMAX // FETCH):

        @pl.when(n * FETCH < live)
        def _(n=n):
            fetch(n).wait()
            step = FETCH // TOGETHER
            lax.fori_loop(n * step, jnp.minimum(whole, (n + 1) * step), add_some, 0)

    lax.fori_loop(whole * TOGETHER, live, add_one, 0)
    multiply(dense.at[pl.ds(AWAY, AWAY)], held, extra, away_out)
    multiply(dense.at[pl.ds(0, AWAY)], held, extra, kept_out)


def first_products(count, rows, cols, ids, adj):
    hbm = pl.BlockSpec(memory_space=pltpu.HBM)
    chunks = jax.ShapeDtypeStruct((4, ROWS, PANEL), jnp.float32)
    dense = jax.ShapeDtypeStruct((DEST_TILES * TILE, SRC_TILES * TILE), jnp.bfloat16)
    arrays = [pltpu.with_memory_space_constraint(x, pltpu.HBM) for x in (rows, cols, ids, adj)]
    return pl.pallas_call(
        first_kernel,
        in_specs=[pl.BlockSpec(memory_space=pltpu.SMEM)] + [hbm] * 4,
        out_specs=[VMEM] * 3,
        out_shape=[chunks, chunks, dense],
        scratch_shapes=[
            pltpu.SMEM((KMAX,), jnp.int32),
            pltpu.SMEM((KMAX,), jnp.int32),
            pltpu.VMEM((1, PANEL), jnp.int32),
            pltpu.VMEM((KMAX, TILE, TILE), jnp.bfloat16),
            pltpu.VMEM((SRC_TILES * TILE, PANEL), jnp.bfloat16),
            pltpu.VMEM((EXTRA, PANEL), jnp.float32),
            pltpu.SemaphoreType.DMA((KMAX // FETCH,)),
            pltpu.SemaphoreType.DMA((3,)),
        ],
        compiler_params=WIDE,
        name="first_products",
    )(count, *arrays)


def away_kernel(dense, sources, out, held, extra):
    parts = jnp.sum(f32(sources[:, TILE:ROWS, :]), axis=0)
    squares = (parts[0:1] + parts[1:2]) + parts[2:3]
    row = lax.broadcasted_iota(jnp.int32, (EXTRA, PANEL), 0)
    extra[...] = jnp.where(row == lax.axis_index("col_1"), jnp.broadcast_to(squares, (EXTRA, PANEL)), 0.0)
    for t in range(SRC_TILES):
        held[t * TILE : (t + 1) * TILE, :] = sources[t, 0:TILE, :]
    multiply(dense.at[pl.ds(AWAY, AWAY)], held, extra, out)


def away_products(dense, sources):
    return pl.pallas_call(
        away_kernel,
        in_specs=[VMEM, VMEM],
        out_specs=[VMEM] * 3,
        out_shape=[
            jax.ShapeDtypeStruct((4, ROWS, PANEL), jnp.float32),
            jax.ShapeDtypeStruct((SRC_TILES * TILE, PANEL), jnp.bfloat16),
            jax.ShapeDtypeStruct((EXTRA, PANEL), jnp.float32),
        ],
        compiler_params=LIMIT,
        name="away_products",
    )(dense, sources)


def kept_kernel(dense, held, extra, out):
    multiply(dense.at[pl.ds(0, AWAY)], held, extra, out)


def kept_products(dense, held, extra):
    return pl.pallas_call(
        kept_kernel,
        in_specs=[VMEM] * 3,
        out_specs=VMEM,
        out_shape=jax.ShapeDtypeStruct((4, ROWS, PANEL), jnp.float32),
        compiler_params=LIMIT,
        name="kept_products",
    )(dense, held, extra)


def as_integers(x):
    x = jnp.maximum(x, 2.0**-80)
    exponent = jnp.floor(jnp.log2(x)) - 22.0
    return jnp.floor(x * jnp.exp2(-exponent) + 0.5), exponent


def encode_kernel(kept, away, beside, far, own):
    row = lax.broadcasted_iota(jnp.int32, (EXTRA, PANEL), 0)
    for k, coded in enumerate((beside.at[0], beside.at[1], far, own)):
        total = kept[k] + away[k]
        sums = total[0:TILE]
        lines = list(as_integers(jnp.max(sums, axis=0, keepdims=True)))
        factor = TOP / jnp.sqrt(jnp.sqrt(lines[0] * jnp.exp2(lines[1])))
        codes = jnp.floor(jnp.sqrt(jnp.sqrt(sums)) * factor + 0.5)
        codes = jnp.minimum(codes, TOP).astype(jnp.int32)
        coded[0:HALF, :] = lax.shift_left(codes[0:HALF], 16) | codes[HALF:TILE]
        lines += as_integers(total[TILE : TILE + 1])
        lines += as_integers(total[TILE + 1 : TILE + 2])
        tail = jnp.zeros((EXTRA, PANEL), jnp.float32)
        for n, line in enumerate(lines):
            tail = jnp.where(row == n, jnp.broadcast_to(line, (EXTRA, PANEL)), tail)
        coded[HALF:CODED, :] = tail.astype(jnp.int32)


def encoded(kept, away):
    return pl.pallas_call(
        encode_kernel,
        in_specs=[VMEM] * 2,
        out_specs=[VMEM] * 3,
        out_shape=[
            jax.ShapeDtypeStruct((2, CODED, PANEL), jnp.int32),
            jax.ShapeDtypeStruct((CODED, PANEL), jnp.int32),
            jax.ShapeDtypeStruct((CODED, PANEL), jnp.int32),
        ],
        compiler_params=LIMIT,
        name="encoded",
    )(kept, away)


def split3(x):
    high = f32(x.astype(jnp.bfloat16))
    rest = x - high
    middle = f32(rest.astype(jnp.bfloat16))
    return high, middle, rest - middle


def fourth_power(codes):
    root = f32(codes) * (1.0 / TOP)
    return (root * root) * (root * root)


def decoded(chunks):
    highs = jnp.zeros((HALF, PANEL), jnp.float32)
    lows = jnp.zeros((HALF, PANEL), jnp.float32)
    shares = []
    for coded in chunks:
        tail = f32(coded[HALF:CODED, :])
        power = jnp.exp2(jnp.minimum(tail, 127.0))
        scale = tail[0:1] * power[1:2]
        shares.append(tail[2:3] * power[3:4] + tail[4:5] * power[5:6])
        codes = coded[0:HALF, :]
        highs = highs + fourth_power(lax.shift_right_logical(codes, 16)) * scale
        lows = lows + fourth_power(codes & 65535) * scale
    return jnp.concatenate([highs, lows], axis=0), shares


def outgoing(paths, out):
    square = jnp.sum(paths * paths, axis=0, keepdims=True)
    if out.shape[0] == 1:
        out[...] = square
        return
    row = lax.broadcasted_iota(jnp.int32, (EXTRA, PANEL), 0)
    tail = jnp.zeros((EXTRA, PANEL), jnp.float32)
    for n, line in enumerate(split3(square)):
        tail = jnp.where(row == n, jnp.broadcast_to(line, (EXTRA, PANEL)), tail)
    out[0:TILE, :] = paths.astype(jnp.bfloat16)
    out[TILE:ROWS, :] = tail.astype(jnp.bfloat16)


def start_piece(ids):
    position = jnp.int32(0)
    for axis, count in zip(ROW_COL, SPLIT):
        position = position * count + lax.axis_index(axis)
    vertex = position * TILE + lax.broadcasted_iota(jnp.int32, (TILE, PANEL), 0)
    return jnp.where(vertex == jnp.broadcast_to(ids[...], (TILE, PANEL)), 1.0, 0.0)


def first_level_kernel(own, far, heard, handed, depth, raw, out):
    product, _ = decoded((own, far, heard.at[0], handed))
    paths = jnp.where(depth[...] >= 1, product, 0.0)
    raw[...] = paths
    outgoing(paths, out)


def level_kernel(level, own, far, heard, handed, depth, raw_in, sums_in, raw, out, sums, scale):
    before = start_piece(sums_in) if level == 2 else sums_in[...]
    product, shares = decoded((own, far, heard.at[0], handed))
    mean_square = jnp.zeros((1, PANEL), jnp.float32)
    turned = 2 * lax.axis_index("col_1")
    back = (0, 2, 1 + turned, 3 - turned)
    for j in range(4):
        for k, share in zip(back, shares):
            here = ((lax.axis_index("col_0") - j) & 3) == k
            mean_square = mean_square + jnp.where(here, share, 0.0)
    mean_square = mean_square / VERTICES + EPSILON
    scale[...] = mean_square
    inverse = lax.rsqrt(mean_square)
    sums[...] = before + raw_in[...] * inverse
    paths = jnp.where(depth[...] >= level, product * inverse, 0.0)
    raw[...] = paths
    outgoing(paths, out)


def finish_level(level, chunks, depth, raw, sums):
    panel = jax.ShapeDtypeStruct((TILE, PANEL), jnp.float32)
    line = jax.ShapeDtypeStruct((1, PANEL), jnp.float32)
    piece = jax.ShapeDtypeStruct((ROWS, PANEL), jnp.bfloat16)
    first = level == 1
    shapes = [panel, piece if level < LEVELS else line] + ([] if first else [panel, line])
    return pl.pallas_call(
        first_level_kernel if first else lambda *refs: level_kernel(level, *refs),
        in_specs=[VMEM] * (5 if first else 7),
        out_specs=[VMEM] * len(shapes),
        out_shape=shapes,
        compiler_params=LIMIT,
    )(*chunks, depth, *(() if first else (raw, sums)))


def from_partner(x):
    return lax.ppermute(x, "col_1", [(0, 1), (1, 0)])


def exchanged(kept, away):
    beside, far, own = encoded(kept, from_partner(away))
    far = lax.ppermute(far, "col_0", [(i, (i + 2) % 4) for i in range(4)])
    forward = [(2 * i, 2 * ((i + 1) % 4)) for i in range(4)]
    backward = [(2 * i + 1, 2 * ((i - 1) % 4) + 1) for i in range(4)]
    heard = lax.ppermute(beside, COL, forward + backward)
    return own, far, heard, from_partner(heard[1])


def everywhere(line, axes):
    copies = jnp.broadcast_to(line, (lax.axis_size(axes), EXTRA, PANEL))
    return lax.all_to_all(copies, axes, 0, 0, tiled=True)


def last_kernel(squares, raw, sums, *refs):
    scales, (path_sums, log_scales) = refs[:-2], refs[-2:]
    total = squares[0, 0:1, :]
    for i in range(1, squares.shape[0]):
        total = total + squares[i, 0:1, :]
    mean_square = total / VERTICES + EPSILON
    path_sums[...] = sums[...] + raw[...] * lax.rsqrt(mean_square)
    for n, scale in enumerate(scales):
        log_scales[n : n + 1, :] = 0.5 * jnp.log(scale[...])
    log_scales[LEVELS - 1 : LEVELS, :] = 0.5 * jnp.log(mean_square)


def last_level(squares, raw, sums, scales):
    return pl.pallas_call(
        last_kernel,
        in_specs=[VMEM] * (3 + len(scales)),
        out_specs=[VMEM] * 2,
        out_shape=[
            jax.ShapeDtypeStruct((TILE, PANEL), jnp.float32),
            jax.ShapeDtypeStruct((LEVELS, PANEL), jnp.float32),
        ],
        compiler_params=LIMIT,
        name="last_level",
    )(squares, raw, sums, *scales)


def local(adj_tiles, tile_rows, tile_cols, tile_count, tile_depth, source_ids):
    away, kept, dense = first_products(
        tile_count, tile_rows[0, 0], tile_cols[0, 0], source_ids[None, :], adj_tiles[0, 0]
    )
    sums = source_ids[None, :]
    raw, piece, *_ = finish_level(1, exchanged(kept, away), tile_depth, None, None)
    scales = []
    for level in range(2, LEVELS + 1):
        spread = jnp.broadcast_to(piece, (SRC_TILES, ROWS, PANEL))
        sources = lax.all_to_all(spread, ROW, 0, 0, tiled=True)
        away, held, extra = away_products(dense, sources)
        chunks = exchanged(kept_products(dense, held, extra), away)
        raw, piece, sums, scale = finish_level(level, chunks, tile_depth, raw, sums)
        scales.append(scale)
    squares = jnp.sum(everywhere(piece, ("row_1",) + COL)[:, 0], axis=0, keepdims=True)
    return tuple(last_level(everywhere(squares, ("row_0", "row_2")), raw, sums, scales))


def solution(mesh):
    split = Mesh(mesh.devices.reshape(SPLIT), ROW_COL)
    in_specs = (
        P(ROW, COL, None, None, None),
        P(ROW, COL, None),
        P(ROW, COL, None),
        P(ROW, COL),
        P(ROW_COL, None),
        P(),
    )
    out_specs = (P(ROW_COL, None), P())
    return jax.shard_map(local, mesh=split, in_specs=in_specs, out_specs=out_specs, check_vma=False)
```
